32 devices in a mesh: rep: 16 (over z, y, core), tp: 2 (over x).
Axes of the slice: x: 2, y: 2, z: 4, core: 2. Of those that a mesh axis runs over, the one named last changes fastest.
Arguments:
- positions: int32 [4096], P('rep'), may hold values from 0 to 8191
- activations: bfloat16 [4096, 4096], P('rep', 'tp'), may hold values from -6 to 6
- norm_gain: bfloat16 [4096], P('tp'), may hold values from 0.5 to 1.5
- qkv_weight: bfloat16 [4096, 6144], P('rep', 'tp'), may hold values from -0.09375 to 0.09375
- gate_up_weight: bfloat16 [4096, 14336], P('rep', 'tp'), may hold values from -0.09375 to 0.09375
Outputs:
- qkv_out: bfloat16 [4096, 6144], P('rep', 'tp')
- hidden: bfloat16 [4096, 7168], P('rep', 'tp')
The draws below stay inside these ranges and needn't reach their ends.
All inputs are finite; a program needn't handle non-finite values.
Results may differ from the reference program's by a relative error of at most 0.0058.
Values may be sent and summed in bfloat16 or wider, within the bound.
A program may use at most 192 MiB of HBM per device.

```python
import jax
import jax.numpy as jnp
from jax import lax

D = 4096
QH = 32
KVH = 8
HD = 128
FF = 7168
QKV = 6144
TOTAL_SEQS = 4096
N_TP = 2


def with_ends(entries, rng, smallest, largest):
    shape = entries.shape
    index_at = [jax.random.randint(jax.random.fold_in(rng, axis), (), 0, shape[axis]) for axis in range(len(shape))]
    entries = entries.at[tuple(index_at)].set(smallest)
    longest = shape.index(max(shape))
    index_at[longest] = (index_at[longest] + 1) % shape[longest]
    return entries.at[tuple(index_at)].set(largest)


def steps_of(rng, extent, pieces, low, largest):
    def one(axis_at, shards_of):
        heights = jax.random.uniform(jax.random.fold_in(jax.random.fold_in(rng, 6), axis_at), (shards_of,), jnp.float32, low / len(pieces), largest / len(pieces))
        return jnp.repeat(jnp.exp(heights), extent[axis_at] // shards_of).reshape((-1,) + (1,) * (len(extent) - axis_at - 1))

    loudness = one(*pieces[0])
    for cut in pieces[1:]:
        loudness = loudness * one(*cut)
    return loudness


def gaussian(key, shape, scale, most, pieces=(), kind=jnp.bfloat16):
    entries = scale * jax.random.normal(key, shape, jnp.float32)
    if pieces:
        entries = entries * steps_of(key, shape, pieces, -0.22, 0.18)
    return jnp.clip(entries, -most, most).astype(kind)


def setup_inputs(seed: int = 0) -> dict:
    seeds = jax.random.split(jax.random.key(seed), 6)
    return {
        "positions": with_ends(jax.random.randint(seeds[0], (TOTAL_SEQS,), 0, 8192), jax.random.fold_in(seeds[0], 1), 0, 8191).astype(jnp.int32),
        "activations": gaussian(seeds[1], (TOTAL_SEQS, D), 1.0, 6.0, ((0, 16), (1, 2))),
        "norm_gain": jnp.clip(1.0 + 0.1 * jax.random.normal(seeds[2], (D,), jnp.float32), 0.5, 1.5).astype(jnp.bfloat16),
        "qkv_weight": gaussian(seeds[3], (D, QKV), D ** -0.5, 0.09375, ((0, 16), (1, 2))),
        "gate_up_weight": gaussian(seeds[4], (D, 2 * FF), D ** -0.5, 0.09375, ((0, 16), (1, 2))),
    }


theta_base = 500000.0
norm_eps = 1e-05

def normalize(gathered, gain_row):
    values = gathered.astype(jnp.float32)
    mean_square = lax.optimization_barrier(jnp.mean(values * values, axis=1, keepdims=True))
    return (values * lax.rsqrt(mean_square + norm_eps) * gain_row.astype(jnp.float32)).astype(jnp.bfloat16)

def rotary(joined_qkv, positions):
    row_count = joined_qkv.shape[0]
    per_group = QH // KVH + 2
    half_size = HD // 2
    head_view = joined_qkv.reshape(row_count, -1, per_group, HD)
    frequency = theta_base ** (-2.0 * jnp.arange(half_size, dtype=jnp.float32) / HD)
    angles = positions.astype(jnp.float32)[:, None] * frequency[None, :]
    cosine = jnp.cos(angles)[:, None, None, :]
    sine_part = jnp.sin(angles)[:, None, None, :]
    leading = head_view[..., :half_size]
    trailing = head_view[..., half_size:]
    turned = jnp.concatenate([leading * cosine - trailing * sine_part, trailing * cosine + leading * sine_part], axis=-1)
    rotated_mask = (jnp.arange(per_group) < per_group - 1)[None, None, :, None]
    return jnp.where(rotated_mask, turned, head_view).reshape(row_count, -1)

def reference(positions, activations, norm_gain, qkv_weight, gate_up_weight):
    normed = normalize(activations, norm_gain)
    joined_qkv = jnp.dot(normed, qkv_weight, preferred_element_type=jnp.float32)
    qkv_out = rotary(joined_qkv, positions).astype(jnp.bfloat16)
    gate_up = jnp.dot(normed, gate_up_weight, preferred_element_type=jnp.float32)
    row_count = gate_up.shape[0]
    paired = gate_up.reshape(row_count, N_TP, 2, FF // N_TP)
    hidden = (jax.nn.silu(paired[:, :, 0]) * paired[:, :, 1]).reshape(row_count, FF).astype(jnp.bfloat16)
    return (qkv_out, hidden)
```

```python
import functools

import jax
import jax.numpy as jnp
from jax import lax
from jax.experimental import pallas as pl
from jax.experimental.pallas import tpu as pltpu
from jax.sharding import PartitionSpec as P

QH = 32
KVH = 8
HD = 128
MESH = pl.DeviceIdType.MESH
CORES = 2
QUARTERS = 4
CHIPS = 8
WINDOW = 4
BACKLOG = 4
PIECES = 4
NEAR_FIRST = 0
WIDE = 2 * HD
OWN, ACROSS = (0, 1, 2, 3), (4, 5, 6, 7)

theta_base = 500000.0
norm_eps = 1e-05


def normalize(gathered, gain_row):
    values = gathered.astype(jnp.float32)
    mean_square = jnp.mean(values * values, axis=1, keepdims=True)
    return (values * lax.rsqrt(mean_square + norm_eps) * gain_row.astype(jnp.float32)).astype(
        jnp.bfloat16
    )


def frequencies():
    half_size = HD // 2
    return theta_base ** (-2.0 * jnp.arange(half_size, dtype=jnp.float32) / HD)


def rotary(joined_qkv, positions):
    row_count = joined_qkv.shape[0]
    per_group = QH // KVH + 2
    half_size = HD // 2
    head_view = joined_qkv.reshape(row_count, -1, per_group, HD)
    angles = positions.astype(jnp.float32)[:, None] * frequencies()[None, :]
    cosine = jnp.cos(angles)[:, None, None, :]
    sine_part = jnp.sin(angles)[:, None, None, :]
    leading = head_view[..., :half_size]
    trailing = head_view[..., half_size:]
    turned = jnp.concatenate(
        [leading * cosine - trailing * sine_part, trailing * cosine + leading * sine_part], axis=-1
    )
    rotated_mask = (jnp.arange(per_group) < per_group - 1)[None, None, :, None]
    return jnp.where(rotated_mask, turned, head_view).reshape(row_count, -1)


def contract_rows(chosen, piece):
    return jnp.dot(chosen, piece, preferred_element_type=jnp.float32)


def plain(positions, activations, norm_gain, qkv_weight, gate_up_weight):
    features, gains = (
        lax.all_gather(activations, "tp", axis=1, tiled=True),
        lax.all_gather(norm_gain, "tp", axis=0, tiled=True),
    )
    normed = normalize(features, gains)
    seq_count = normed.shape[0]
    qkv_partial = contract_rows(normed, lax.all_gather(qkv_weight, "rep", axis=0, tiled=True))
    gateup_partial = contract_rows(
        normed, lax.all_gather(gate_up_weight, "rep", axis=0, tiled=True)
    )
    qkv_out = rotary(qkv_partial, positions).astype(jnp.bfloat16)
    paired = gateup_partial.reshape(seq_count, 2, -1)
    hidden = (jax.nn.silu(paired[:, 0]) * paired[:, 1]).astype(jnp.bfloat16)
    return (qkv_out, hidden)


def kernel(plan, pos_in, freq_in, x_in, gain_in, wq_in, wg_in, q_out, h_out, *scratch):
    (seqs, feats, qcols, hcols) = plan
    n_q, n_h = qcols // WIDE, hcols // HD
    n = n_q + n_h
    (x_buf, t_buf, g_buf, f_buf, acc) = scratch[:5]
    p_buf = scratch[5:9]
    w_buf = scratch[9 : 9 + n]
    res = scratch[9 + n : 9 + 2 * n]
    (w_send, w_recv, f_send, f_recv, o_send, o_recv, a_send, a_recv, l_sem, ready) = scratch[9 + 2 * n :]
    last = n - 1

    rep, t = lax.axis_index("rep"), lax.axis_index("tp")
    core = rep % CORES
    chip = rep // CORES
    half = chip // QUARTERS
    quarter = chip % QUARTERS
    zl, y = quarter // 2, quarter % 2
    inner = (half + zl) % 2 == 1

    def flip_quarter(j):
        return (zl + j // 2 % 2) % 2 * 2 + (y + j % 2) % 2

    def flip(j):
        return (half + j // 4) % 2 * QUARTERS + flip_quarter(j)

    def dev(other_chip, other_core=None, other_t=None):
        return (
            other_chip * CORES + (core if other_core is None else other_core),
            t if other_t is None else other_t,
        )

    sibling = dev(chip, 1 - core)
    across = dev(chip, core, 1 - t)
    y_peer, z_peer, middle = dev(flip(1)), dev(flip(2)), dev(flip(6))

    def remote(src, dst, ssem, rsem, where):
        return pltpu.make_async_remote_copy(
            src_ref=src, dst_ref=dst, send_sem=ssem, recv_sem=rsem, device_id=where, device_id_type=MESH
        )

    def signal(sem, where):
        pl.semaphore_signal(sem, inc=1, device_id=where, device_id_type=MESH)

    def rows(index, count=1):
        return pl.ds(pl.multiple_of(index * seqs, seqs), count * seqs)

    def cols(base, width):
        return pl.ds(pl.multiple_of(base, HD), width)

    barrier = pltpu.get_barrier_semaphore()
    for where in (sibling, across, y_peer):
        signal(barrier, where)

    @pl.when(inner)
    def _():
        signal(barrier, middle)
        signal(barrier, z_peer)

    mine = cols(t * feats, feats)

    def mine_at(j):
        return x_buf.at[rows(flip_quarter(j)), mine]

    local = [
        pltpu.make_async_copy(x_in, mine_at(0), l_sem.at[0]),
        pltpu.make_async_copy(pos_in, p_buf[0], l_sem.at[1]),
        pltpu.make_async_copy(gain_in, g_buf.at[mine], l_sem.at[2]),
        pltpu.make_async_copy(freq_in, f_buf, l_sem.at[3]),
    ]
    for copy in local:
        copy.start()

    part_rows = seqs // PIECES

    def held(j, p):
        return x_buf.at[pl.ds(pl.multiple_of(flip_quarter(j) * seqs + p * part_rows, part_rows), part_rows), mine]

    def fresh(p):
        return x_in.at[p * part_rows : (p + 1) * part_rows, :]

    def act(n, src, j, where):
        return [
            remote(src(p), held(j, p), a_send.at[n, p], a_recv.at[n, p], where) for p in range(PIECES)
        ]

    z_x = act(0, fresh, 0, z_peer)
    y_x = act(1, fresh, 0, y_peer)
    y_two = act(2, functools.partial(held, 2), 2, y_peer)
    x_own = act(3, fresh, 0, across)
    x_two = act(4, functools.partial(held, 2), 2, across)
    x_three = act(5, functools.partial(held, 1), 1, across)
    x_four = act(6, functools.partial(held, 3), 3, across)
    x_gain = remote(gain_in, g_buf.at[mine], a_send.at[7, 0], a_recv.at[7, 0], across)
    p_far = [remote(pos_in, p_buf[j], a_send.at[7 + j, 0], a_recv.at[7 + j, 0], dev(flip(j))) for j in (1, 2, 3)]

    def sources(c, q):
        if c < n_q:
            return [wq_in.at[:, cols(q * qcols + c * WIDE, WIDE)]]
        at = q * hcols + (c - n_q) * HD
        return [wg_in.at[:, cols(part * hcols * QUARTERS + at, HD)] for part in range(2)]

    def slab(c, owner):
        return w_buf[c].at[rows(owner), :]

    def parts(c, owner):
        if c < n_q:
            return [slab(c, owner)]
        return [w_buf[c].at[rows(owner), part * HD : (part + 1) * HD] for part in range(2)]

    def weight_start(c, j):
        for src, dst in zip(sources(c, flip_quarter(j)), parts(c, rep)):
            remote(src, dst, w_send.at[c, j], w_recv.at[c, j], dev(flip(j))).start()

    def weight(c, j):
        place = slab(c, flip(j) * CORES + core)
        return remote(place, place, w_send.at[c, j], w_recv.at[c, j], dev(flip(j)))

    def start_own(c):
        for src, dst in zip(sources(c, quarter), parts(c, rep)):
            pltpu.make_async_copy(src, dst, l_sem.at[4 + c]).start()
            remote(src, dst, f_send.at[c, 0], f_recv.at[c, 0], sibling).start()

    def own_wait(c):
        place = slab(c, rep)
        pltpu.make_async_copy(place, place, l_sem.at[4 + c]).wait()

    def passed(c, j):
        place = slab(c, flip(j) * CORES + core)
        return remote(place, place, f_send.at[c, j], f_recv.at[c, j], sibling)

    def passed_in(c, j):
        place = slab(c, flip(j) * CORES + 1 - core)
        return remote(place, place, f_send.at[c, j], f_recv.at[c, j], sibling)

    def start_near(c):
        for j in OWN[1:]:
            weight_start(c, j)
        start_own(c)

    def start_far(c):
        for j in ACROSS:
            weight_start(c, j)

    def take(c, js):
        for j in js:
            if j:
                weight(c, j).wait_recv()
                passed(c, j).start()

    def settle(c, js):
        for j in js:
            if j == 0:
                own_wait(c)
            passed_in(c, j).wait_recv()

    def advance(c):
        if c + WINDOW < n:
            for j in ACROSS:
                weight(c, j).wait_send()
                weight_start(c + WINDOW, j)

    pl.semaphore_wait(barrier, 4)

    @pl.when(inner)
    def _():
        weight_start(0, 6)

    for copy in (*x_own, *y_x, x_gain):
        copy.start()

    @pl.when(inner)
    def _():
        pl.semaphore_wait(ready.at[0], 1)
        signal(ready.at[1], middle)
        for copy in z_x:
            copy.start()
        pl.semaphore_wait(ready.at[1], 1)
        signal(ready.at[2], z_peer)

    @pl.when(jnp.logical_not(inner))
    def _():
        signal(ready.at[0], z_peer)
        for copy in z_x:
            copy.start()
        pl.semaphore_wait(ready.at[2], 1)
        weight_start(0, 6)

    for copy in p_far:
        copy.start()
    for j in (4, 5, 7):
        weight_start(0, j)
    for c in range(1, WINDOW):
        start_far(c)
    for c in range(NEAR_FIRST):
        start_near(c)
    for p in range(PIECES):
        z_x[p].wait_recv()
        x_two[p].start()
        y_two[p].start()
    for p in range(PIECES):
        y_x[p].wait_recv()
        x_three[p].start()
    for c in range(NEAR_FIRST, n):
        start_near(c)
    for p in range(PIECES):
        y_two[p].wait_recv()
        x_four[p].start()
    for c in range(BACKLOG):
        take(c, OWN + ACROSS)
        advance(c)

    for copy in local:
        copy.wait()
    for copy in p_far:
        copy.wait_recv()

    freq = f_buf[...]
    for j in range(QUARTERS):
        for s in range(seqs // HD):
            line = p_buf[j][s * HD : (s + 1) * HD].astype(jnp.float32)[None, :]
            angles = jnp.transpose(jnp.broadcast_to(line, (HD, HD))) * freq
            at_rows = pl.ds(pl.multiple_of(flip_quarter(j) * seqs + s * HD, HD), HD)
            t_buf[at_rows, :HD] = jnp.cos(angles)
            lane = lax.broadcasted_iota(jnp.int32, angles.shape, 1)
            sines = jnp.sin(angles)
            t_buf[at_rows, HD:] = jnp.where(lane < HD // 2, -sines, sines)

    tall = 32
    x_gain.wait_recv()
    gain_row = g_buf[...].astype(jnp.float32)[None, :]

    for j, copies in ((0, x_own), (2, x_two), (1, x_three), (3, x_four)):
        for copy in copies:
            copy.wait_recv()
        for copy in {0: (*z_x, *y_x, *x_own, x_gain, *p_far), 2: (*y_two, *x_two), 1: x_three, 3: x_four}[j]:
            copy.wait_send()

        @pl.loop(0, seqs // tall)
        def _(i):
            at_rows = pl.ds(pl.multiple_of(flip_quarter(j) * seqs + i * tall, tall), tall)
            values = x_buf[at_rows, :].astype(jnp.float32)
            mean_square = jnp.mean(values * values, axis=1, keepdims=True)
            x_buf[at_rows, :] = (values * lax.rsqrt(mean_square + norm_eps) * gain_row).astype(jnp.bfloat16)

    total = QUARTERS * seqs
    per_group = QH // KVH + 2
    deep = 2 * seqs

    def turn(c, at_rows, wide):
        for s in range(WIDE // HD):
            head = wide[:, s * HD : (s + 1) * HD]
            if (c * (WIDE // HD) + s) % per_group < per_group - 1:
                head = head * t_buf[at_rows, :HD] + pltpu.roll(head, HD // 2, 1) * t_buf[at_rows, HD:]
            res[c][at_rows, s * HD : (s + 1) * HD] = head.astype(jnp.bfloat16)

    def gated(c, at_rows, wide):
        gate, up = wide[:, :HD], wide[:, HD:]
        res[c][at_rows, :] = (gate / (1.0 + jnp.exp(-gate)) * up).astype(jnp.bfloat16)

    def compute(c):
        @pl.loop(0, total // deep)
        def _(i):
            at_rows = pl.ds(pl.multiple_of(i * deep, deep), deep)
            wide = jnp.dot(x_buf[at_rows, :], w_buf[c][...], preferred_element_type=jnp.float32)
            (turn if c < n_q else gated)(c, at_rows, wide)

    def back(c, j):
        src = res[c].at[rows(flip_quarter(j)), :]
        if c < n_q:
            dst = q_out.at[:, cols(quarter * qcols + c * WIDE, WIDE)]
        else:
            dst = h_out.at[:, cols(quarter * hcols + (c - n_q) * HD, HD)]
        return src, dst

    def back_send(c, j):
        src, dst = back(c, j)
        return remote(src, dst, o_send.at[c, j], o_recv.at[c, j], dev(flip(j)))

    def back_from(c, j):
        mover = flip_quarter(j)
        if c < n_q:
            dst = q_out.at[:, cols(mover * qcols + c * WIDE, WIDE)]
        else:
            dst = h_out.at[:, cols(mover * hcols + (c - n_q) * HD, HD)]
        return remote(dst, dst, o_send.at[c, j], o_recv.at[c, j], dev(flip(j)))

    def back_own(c):
        return pltpu.make_async_copy(*back(c, 0), o_send.at[c, 0])

    def ship(c, js=(3, 1, 2, 0)):
        for j in js:
            (back_send(c, j) if j else back_own(c)).start()

    for c in range(n - 1):
        if c >= BACKLOG:
            take(c, OWN + ACROSS)
            advance(c)
        settle(c, OWN + ACROSS)
        compute(c)
        ship(c)

    deep_half = QUARTERS * CORES * seqs
    near = pl.ds(pl.multiple_of(half * deep_half, deep_half), deep_half)
    far = pl.ds(pl.multiple_of((1 - half) * deep_half, deep_half), deep_half)
    take(last, OWN)
    settle(last, OWN)

    @pl.loop(0, total // deep)
    def _(i):
        at_rows = pl.ds(pl.multiple_of(i * deep, deep), deep)
        acc[at_rows, :] = jnp.dot(x_buf[at_rows, near], w_buf[last][near, :], preferred_element_type=jnp.float32)
    take(last, ACROSS)
    settle(last, ACROSS)
    for j in (3, 1, 2, 0):
        at_rows = rows(flip_quarter(j))
        gated(
            last,
            at_rows,
            acc[at_rows, :]
            + jnp.dot(x_buf[at_rows, far], w_buf[last][far, :], preferred_element_type=jnp.float32),
        )
        ship(last, (j,))
    for c in range(n):
        for j in OWN + ACROSS:
            if j and (c + WINDOW >= n or j < QUARTERS):
                weight(c, j).wait_send()
            if j:
                passed(c, j).wait_send()
        own_slab = slab(c, rep)
        remote(own_slab, own_slab, f_send.at[c, 0], f_recv.at[c, 0], sibling).wait_send()
        for j in OWN[1:]:
            back_send(c, j).wait_send()
            back_from(c, j).wait_recv()
        back_own(c).wait()


def fused(positions, activations, norm_gain, qkv_weight, gate_up_weight):
    seqs, feats = activations.shape
    depth, qkv_cols = qkv_weight.shape
    qcols = qkv_cols // QUARTERS
    hcols = gate_up_weight.shape[1] // 2 // QUARTERS
    n_q, n_h = qcols // WIDE, hcols // HD
    n = n_q + n_h
    rank = CHIPS * CORES
    freq = frequencies()
    freq = jnp.concatenate([freq, freq])[None, :]
    bf16, f32 = jnp.bfloat16, jnp.float32
    dma = pltpu.SemaphoreType.DMA
    total = QUARTERS * seqs
    scratch = [
        pltpu.VMEM((total, 2 * feats), bf16),
        pltpu.VMEM((total, 2 * HD), f32),
        pltpu.VMEM((2 * feats,), bf16),
        pltpu.VMEM((1, HD), f32),
        pltpu.VMEM((total, WIDE), f32),
        *[pltpu.VMEM((seqs,), jnp.int32) for _ in range(QUARTERS)],
        *[pltpu.VMEM((rank * depth, WIDE), bf16) for _ in range(n)],
        *[pltpu.VMEM((total, WIDE), bf16) for _ in range(n_q)],
        *[pltpu.VMEM((total, HD), bf16) for _ in range(n_h)],
        dma((n, CHIPS)),
        dma((n, CHIPS)),
        dma((n, CHIPS)),
        dma((n, CHIPS)),
        dma((n, QUARTERS)),
        dma((n, QUARTERS)),
        dma((11, PIECES)),
        dma((11, PIECES)),
        dma((4 + n,)),
        pltpu.SemaphoreType.REGULAR((3,)),
    ]
    plan = (seqs, feats, qcols, hcols)
    anywhere = pl.BlockSpec(memory_space=pl.ANY)
    return pl.pallas_call(
        functools.partial(kernel, plan),
        out_shape=(
            pltpu.VMEM((seqs, qkv_cols), bf16),
            pltpu.VMEM((seqs, hcols * QUARTERS), bf16),
        ),
        in_specs=[anywhere] * 6,
        out_specs=(pl.BlockSpec(memory_space=pltpu.VMEM), pl.BlockSpec(memory_space=pltpu.VMEM)),
        scratch_shapes=scratch,
        compiler_params=pltpu.CompilerParams(
            collective_id=0, has_side_effects=True, vmem_limit_bytes=60 * 1024 * 1024
        ),
    )(positions, freq, activations, norm_gain, qkv_weight, gate_up_weight)


def per_device(reps, tps, positions, activations, norm_gain, qkv_weight, gate_up_weight):
    seqs, depth = activations.shape[0], qkv_weight.shape[0]
    fits = (
        reps == CHIPS * CORES
        and tps == 2
        and seqs == depth
        and seqs % HD == 0
        and qkv_weight.shape[1] % (QUARTERS * (QH // KVH + 2) * HD) == 0
        and gate_up_weight.shape[1] % (2 * QUARTERS * HD) == 0
    )
    step = fused if fits else plain
    return step(positions, activations, norm_gain, qkv_weight, gate_up_weight)


def solution(mesh):
    placed = (P("rep"), P("rep", "tp"), P("tp"), P("rep", "tp"), P("rep", "tp"))
    return jax.shard_map(
        functools.partial(per_device, mesh.shape["rep"], mesh.shape["tp"]),
        mesh=mesh,
        in_specs=placed,
        out_specs=(P("rep", "tp"), P("rep", "tp")),
        check_vma=False,
    )
```

```python
import functools
import math

import jax
import jax.numpy as jnp
from jax import lax
from jax.experimental import pallas as pl
from jax.experimental.pallas import tpu as pltpu
from jax.sharding import PartitionSpec as P

QH = 32
KVH = 8
HD = 128
MESH = pl.DeviceIdType.MESH
CORES = 2
QUARTERS = 4
CHIPS = 8
WINDOW = 4
BACKLOG = 4
PIECES = 4
NEAR_FIRST = 0
WIDE = 2 * HD
ACROSS = (4, 5, 6, 7)
NEAR_LEAD = 0
EARLY = 2
OWN = (0, 1, 2, 3)

theta_base = 500000.0
norm_eps = 1e-05


def normalize(gathered, gain_row):
    values = gathered.astype(jnp.float32)
    mean_square = jnp.mean(values * values, axis=1, keepdims=True)
    return (values * lax.rsqrt(mean_square + norm_eps) * gain_row.astype(jnp.float32)).astype(
        jnp.bfloat16
    )


def frequencies():
    half_size = HD // 2
    return theta_base ** (-2.0 * jnp.arange(half_size, dtype=jnp.float32) / HD)


def rotary(joined_qkv, positions):
    row_count = joined_qkv.shape[0]
    per_group = QH // KVH + 2
    half_size = HD // 2
    head_view = joined_qkv.reshape(row_count, -1, per_group, HD)
    angles = positions.astype(jnp.float32)[:, None] * frequencies()[None, :]
    cosine = jnp.cos(angles)[:, None, None, :]
    sine_part = jnp.sin(angles)[:, None, None, :]
    leading = head_view[..., :half_size]
    trailing = head_view[..., half_size:]
    turned = jnp.concatenate(
        [leading * cosine - trailing * sine_part, trailing * cosine + leading * sine_part], axis=-1
    )
    rotated_mask = (jnp.arange(per_group) < per_group - 1)[None, None, :, None]
    return jnp.where(rotated_mask, turned, head_view).reshape(row_count, -1)


def contract_rows(chosen, piece):
    return jnp.dot(chosen, piece, preferred_element_type=jnp.float32)


def plain(positions, activations, norm_gain, qkv_weight, gate_up_weight):
    features, gains = (
        lax.all_gather(activations, "tp", axis=1, tiled=True),
        lax.all_gather(norm_gain, "tp", axis=0, tiled=True),
    )
    normed = normalize(features, gains)
    seq_count = normed.shape[0]
    qkv_partial = contract_rows(normed, lax.all_gather(qkv_weight, "rep", axis=0, tiled=True))
    gateup_partial = contract_rows(
        normed, lax.all_gather(gate_up_weight, "rep", axis=0, tiled=True)
    )
    qkv_out = rotary(qkv_partial, positions).astype(jnp.bfloat16)
    paired = gateup_partial.reshape(seq_count, 2, -1)
    hidden = (jax.nn.silu(paired[:, 0]) * paired[:, 1]).astype(jnp.bfloat16)
    return (qkv_out, hidden)


def kernel(plan, pos_in, x_in, gain_in, wq_in, wg_in, q_out, h_out, *scratch):
    (seqs, feats, qcols, hcols) = plan
    n_q, n_h = qcols // WIDE, hcols // HD
    n = n_q + n_h
    (x_buf, t_buf, g_buf, acc) = scratch[:4]
    p_buf = scratch[4:8]
    w_buf = scratch[8 : 8 + n]
    res = scratch[8 + n : 8 + 2 * n]
    (w_send, w_recv, f_send, f_recv, o_send, o_recv, a_send, a_recv, l_sem, ready) = scratch[8 + 2 * n :]
    last = n - 1

    rep, t = lax.axis_index("rep"), lax.axis_index("tp")
    core = rep % CORES
    chip = rep // CORES
    half = chip // QUARTERS
    quarter = chip % QUARTERS
    zl, y = quarter // 2, quarter % 2
    inner = (half + zl) % 2 == 1

    def flip_quarter(j):
        return (zl + j // 2 % 2) % 2 * 2 + (y + j % 2) % 2

    def flip(j):
        return (half + j // 4) % 2 * QUARTERS + flip_quarter(j)

    def dev(other_chip, other_core=None, other_t=None):
        return (
            other_chip * CORES + (core if other_core is None else other_core),
            t if other_t is None else other_t,
        )

    sibling = dev(chip, 1 - core)
    across = dev(chip, core, 1 - t)
    y_peer, z_peer, middle = dev(flip(1)), dev(flip(2)), dev(flip(6))

    def remote(src, dst, ssem, rsem, where):
        return pltpu.make_async_remote_copy(
            src_ref=src, dst_ref=dst, send_sem=ssem, recv_sem=rsem, device_id=where, device_id_type=MESH
        )

    def signal(sem, where):
        pl.semaphore_signal(sem, inc=1, device_id=where, device_id_type=MESH)

    def rows(index, count=1):
        return pl.ds(pl.multiple_of(index * seqs, seqs), count * seqs)

    def cols(base, width):
        return pl.ds(pl.multiple_of(base, HD), width)

    barrier = pltpu.get_barrier_semaphore()
    for where in (sibling, across, y_peer):
        signal(barrier, where)

    @pl.when(inner)
    def _():
        signal(barrier, middle)
        signal(barrier, z_peer)

    mine = cols(t * feats, feats)

    def mine_at(j):
        return x_buf.at[rows(flip_quarter(j)), mine]

    local = [
        pltpu.make_async_copy(x_in, mine_at(0), l_sem.at[0]),
        pltpu.make_async_copy(pos_in, p_buf[0], l_sem.at[1]),
        pltpu.make_async_copy(gain_in, g_buf.at[mine], l_sem.at[2]),
    ]
    for copy in local:
        copy.start()

    part_rows = seqs // PIECES

    def held(j, p):
        return x_buf.at[pl.ds(pl.multiple_of(flip_quarter(j) * seqs + p * part_rows, part_rows), part_rows), mine]

    def fresh(p):
        return x_in.at[p * part_rows : (p + 1) * part_rows, :]

    def act(n, src, j, where):
        return [
            remote(src(p), held(j, p), a_send.at[n, p], a_recv.at[n, p], where) for p in range(PIECES)
        ]

    z_x = act(0, fresh, 0, z_peer)
    y_x = act(1, fresh, 0, y_peer)
    y_two = act(2, functools.partial(held, 2), 2, y_peer)
    x_own = act(3, fresh, 0, across)
    x_two = act(4, functools.partial(held, 2), 2, across)
    x_three = act(5, functools.partial(held, 1), 1, across)
    x_four = act(6, functools.partial(held, 3), 3, across)
    x_gain = remote(gain_in, g_buf.at[mine], a_send.at[7, 0], a_recv.at[7, 0], across)
    p_far = [remote(pos_in, p_buf[j], a_send.at[7 + j, 0], a_recv.at[7 + j, 0], dev(flip(j))) for j in (1, 2, 3)]

    def sources(c, q):
        if c < n_q:
            return [wq_in.at[:, cols(q * qcols + c * WIDE, WIDE)]]
        at = q * hcols + (c - n_q) * HD
        return [wg_in.at[:, cols(part * hcols * QUARTERS + at, HD)] for part in range(2)]

    def slab(c, owner):
        return w_buf[c].at[rows(owner), :]

    def parts(c, owner):
        if c < n_q:
            return [slab(c, owner)]
        return [w_buf[c].at[rows(owner), part * HD : (part + 1) * HD] for part in range(2)]

    def weight_start(c, j):
        for src, dst in zip(sources(c, flip_quarter(j)), parts(c, rep)):
            remote(src, dst, w_send.at[c, j], w_recv.at[c, j], dev(flip(j))).start()

    def weight(c, j):
        place = slab(c, flip(j) * CORES + core)
        return remote(place, place, w_send.at[c, j], w_recv.at[c, j], dev(flip(j)))

    def start_own(c):
        for src, dst in zip(sources(c, quarter), parts(c, rep)):
            pltpu.make_async_copy(src, dst, l_sem.at[4 + c]).start()
            remote(src, dst, f_send.at[c, 0], f_recv.at[c, 0], sibling).start()

    def own_wait(c):
        place = slab(c, rep)
        pltpu.make_async_copy(place, place, l_sem.at[4 + c]).wait()

    def passed(c, j):
        place = slab(c, flip(j) * CORES + core)
        return remote(place, place, f_send.at[c, j], f_recv.at[c, j], sibling)

    def passed_in(c, j):
        place = slab(c, flip(j) * CORES + 1 - core)
        return remote(place, place, f_send.at[c, j], f_recv.at[c, j], sibling)

    def start_near(c):
        for j in OWN[1:]:
            weight_start(c, j)
        start_own(c)

    def start_far(c):
        for j in ACROSS:
            weight_start(c, j)

    def take(c, js):
        for j in js:
            if j:
                weight(c, j).wait_recv()
                passed(c, j).start()

    def settle(c, js):
        for j in js:
            if j == 0:
                own_wait(c)
            passed_in(c, j).wait_recv()

    def advance(c):
        if c + WINDOW < n:
            for j in ACROSS:
                weight(c, j).wait_send()
                weight_start(c + WINDOW, j)
                near = j - 4
                if near and c + WINDOW + NEAR_LEAD < n:
                    weight_start(c + WINDOW + NEAR_LEAD, near)
            if c + WINDOW + NEAR_LEAD < n:
                start_own(c + WINDOW + NEAR_LEAD)

    pl.semaphore_wait(barrier, 4)

    @pl.when(inner)
    def _():
        for c in range(EARLY):
            weight_start(c, 6)

    for copy in (*x_own, *y_x, x_gain):
        copy.start()

    @pl.when(inner)
    def _():
        pl.semaphore_wait(ready.at[0], 1)
        signal(ready.at[1], middle)
        for copy in z_x:
            copy.start()
        pl.semaphore_wait(ready.at[1], 1)
        signal(ready.at[2], z_peer)

    @pl.when(jnp.logical_not(inner))
    def _():
        signal(ready.at[0], z_peer)
        for copy in z_x:
            copy.start()
        pl.semaphore_wait(ready.at[2], 1)
        for c in range(EARLY):
            weight_start(c, 6)

    for copy in p_far:
        copy.start()
    for c in range(WINDOW):
        for j in ACROSS:
            if j != 6 or c >= EARLY:
                weight_start(c, j)
    for c in range(NEAR_FIRST):
        start_near(c)

    for p in range(PIECES):
        z_x[p].wait_recv()
        x_two[p].start()
        y_two[p].start()
    for p in range(PIECES):
        y_x[p].wait_recv()
        x_three[p].start()
    for c in range(NEAR_FIRST, n):
        if c < WINDOW + NEAR_LEAD:
            start_near(c)
    for p in range(PIECES):
        y_two[p].wait_recv()
        x_four[p].start()
    for c in range(BACKLOG):
        take(c, OWN + ACROSS)
        advance(c)

    for copy in local:
        copy.wait()
    for copy in p_far:
        copy.wait_recv()

    entry = lax.broadcasted_iota(jnp.int32, (1, HD), 1) % (HD // 2)
    freq = jnp.exp(entry.astype(jnp.float32) * (-2.0 / HD * math.log(theta_base)))
    for j in range(QUARTERS):
        for s in range(seqs // HD):
            line = p_buf[j][s * HD : (s + 1) * HD].astype(jnp.float32)[None, :]
            angles = jnp.transpose(jnp.broadcast_to(line, (HD, HD))) * freq
            at_rows = pl.ds(pl.multiple_of(flip_quarter(j) * seqs + s * HD, HD), HD)
            t_buf[at_rows, :HD] = jnp.cos(angles)
            lane = lax.broadcasted_iota(jnp.int32, angles.shape, 1)
            sines = jnp.sin(angles)
            t_buf[at_rows, HD:] = jnp.where(lane < HD // 2, -sines, sines)

    tall = 32
    x_gain.wait_recv()
    gain_row = g_buf[...].astype(jnp.float32)[None, :]

    for j, copies in ((0, x_own), (2, x_two), (1, x_three), (3, x_four)):
        for copy in copies:
            copy.wait_recv()
        for copy in {0: (*z_x, *y_x, *x_own, x_gain, *p_far), 2: (*y_two, *x_two), 1: x_three, 3: x_four}[j]:
            copy.wait_send()

        @pl.loop(0, seqs // tall)
        def _(i):
            at_rows = pl.ds(pl.multiple_of(flip_quarter(j) * seqs + i * tall, tall), tall)
            values = x_buf[at_rows, :].astype(jnp.float32)
            mean_square = jnp.mean(values * values, axis=1, keepdims=True)
            x_buf[at_rows, :] = (values * lax.rsqrt(mean_square + norm_eps) * gain_row).astype(jnp.bfloat16)

    total = QUARTERS * seqs
    per_group = QH // KVH + 2
    deep = 2 * seqs

    def turn(c, at_rows, wide):
        for s in range(WIDE // HD):
            head = wide[:, s * HD : (s + 1) * HD]
            if (c * (WIDE // HD) + s) % per_group < per_group - 1:
                head = head * t_buf[at_rows, :HD] + pltpu.roll(head, HD // 2, 1) * t_buf[at_rows, HD:]
            res[c][at_rows, s * HD : (s + 1) * HD] = head.astype(jnp.bfloat16)

    def gated(c, at_rows, wide):
        gate, up = wide[:, :HD], wide[:, HD:]
        res[c][at_rows, :] = (gate / (1.0 + jnp.exp(-gate)) * up).astype(jnp.bfloat16)

    def compute(c):
        @pl.loop(0, total // deep)
        def _(i):
            at_rows = pl.ds(pl.multiple_of(i * deep, deep), deep)
            wide = jnp.dot(x_buf[at_rows, :], w_buf[c][...], preferred_element_type=jnp.float32)
            (turn if c < n_q else gated)(c, at_rows, wide)

    def back(c, j):
        src = res[c].at[rows(flip_quarter(j)), :]
        if c < n_q:
            dst = q_out.at[:, cols(quarter * qcols + c * WIDE, WIDE)]
        else:
            dst = h_out.at[:, cols(quarter * hcols + (c - n_q) * HD, HD)]
        return src, dst

    def back_send(c, j):
        src, dst = back(c, j)
        return remote(src, dst, o_send.at[c, j], o_recv.at[c, j], dev(flip(j)))

    def back_from(c, j):
        mover = flip_quarter(j)
        if c < n_q:
            dst = q_out.at[:, cols(mover * qcols + c * WIDE, WIDE)]
        else:
            dst = h_out.at[:, cols(mover * hcols + (c - n_q) * HD, HD)]
        return remote(dst, dst, o_send.at[c, j], o_recv.at[c, j], dev(flip(j)))

    def back_own(c):
        return pltpu.make_async_copy(*back(c, 0), o_send.at[c, 0])

    def ship(c, js=(3, 1, 2, 0)):
        for j in js:
            (back_send(c, j) if j else back_own(c)).start()

    for c in range(n - 1):
        if c >= BACKLOG:
            take(c, OWN + ACROSS)
            advance(c)
        settle(c, OWN + ACROSS)
        compute(c)
        ship(c)

    deep_half = QUARTERS * CORES * seqs
    near = pl.ds(pl.multiple_of(half * deep_half, deep_half), deep_half)
    far = pl.ds(pl.multiple_of((1 - half) * deep_half, deep_half), deep_half)
    take(last, OWN)
    settle(last, OWN)

    @pl.loop(0, total // deep)
    def _(i):
        at_rows = pl.ds(pl.multiple_of(i * deep, deep), deep)
        acc[at_rows, :] = jnp.dot(x_buf[at_rows, near], w_buf[last][near, :], preferred_element_type=jnp.float32)

    take(last, ACROSS)
    settle(last, ACROSS)
    for j in (3, 1, 2, 0):
        at_rows = rows(flip_quarter(j))
        gated(
            last,
            at_rows,
            acc[at_rows, :]
            + jnp.dot(x_buf[at_rows, far], w_buf[last][far, :], preferred_element_type=jnp.float32),
        )
        ship(last, (j,))

    for c in range(n):
        for j in OWN + ACROSS:
            if j and (c + WINDOW >= n or j < QUARTERS):
                weight(c, j).wait_send()
            if j:
                passed(c, j).wait_send()
        own_slab = slab(c, rep)
        remote(own_slab, own_slab, f_send.at[c, 0], f_recv.at[c, 0], sibling).wait_send()
        for j in OWN[1:]:
            back_send(c, j).wait_send()
            back_from(c, j).wait_recv()
        back_own(c).wait()


def fused(positions, activations, norm_gain, qkv_weight, gate_up_weight):
    seqs, feats = activations.shape
    depth, qkv_cols = qkv_weight.shape
    qcols = qkv_cols // QUARTERS
    hcols = gate_up_weight.shape[1] // 2 // QUARTERS
    n_q, n_h = qcols // WIDE, hcols // HD
    n = n_q + n_h
    rank = CHIPS * CORES
    bf16, f32 = jnp.bfloat16, jnp.float32
    dma = pltpu.SemaphoreType.DMA
    total = QUARTERS * seqs
    scratch = [
        pltpu.VMEM((total, 2 * feats), bf16),
        pltpu.VMEM((total, 2 * HD), f32),
        pltpu.VMEM((2 * feats,), bf16),
        pltpu.VMEM((total, WIDE), f32),
        *[pltpu.VMEM((seqs,), jnp.int32) for _ in range(QUARTERS)],
        *[pltpu.VMEM((rank * depth, WIDE), bf16) for _ in range(n)],
        *[pltpu.VMEM((total, WIDE), bf16) for _ in range(n_q)],
        *[pltpu.VMEM((total, HD), bf16) for _ in range(n_h)],
        dma((n, CHIPS)),
        dma((n, CHIPS)),
        dma((n, CHIPS)),
        dma((n, CHIPS)),
        dma((n, QUARTERS)),
        dma((n, QUARTERS)),
        dma((11, PIECES)),
        dma((11, PIECES)),
        dma((4 + n,)),
        pltpu.SemaphoreType.REGULAR((3,)),
    ]
    plan = (seqs, feats, qcols, hcols)
    anywhere = pl.BlockSpec(memory_space=pl.ANY)
    return pl.pallas_call(
        functools.partial(kernel, plan),
        out_shape=(
            pltpu.VMEM((seqs, qkv_cols), bf16),
            pltpu.VMEM((seqs, hcols * QUARTERS), bf16),
        ),
        in_specs=[anywhere] * 5,
        out_specs=(pl.BlockSpec(memory_space=pltpu.VMEM), pl.BlockSpec(memory_space=pltpu.VMEM)),
        scratch_shapes=scratch,
        compiler_params=pltpu.CompilerParams(
            collective_id=0, has_side_effects=True, vmem_limit_bytes=60 * 1024 * 1024
        ),
    )(positions, activations, norm_gain, qkv_weight, gate_up_weight)


def per_device(reps, tps, positions, activations, norm_gain, qkv_weight, gate_up_weight):
    seqs, depth = activations.shape[0], qkv_weight.shape[0]
    fits = (
        reps == CHIPS * CORES
        and tps == 2
        and seqs == depth
        and seqs % HD == 0
        and qkv_weight.shape[1] % (QUARTERS * (QH // KVH + 2) * HD) == 0
        and gate_up_weight.shape[1] % (2 * QUARTERS * HD) == 0
    )
    step = fused if fits else plain
    return step(positions, activations, norm_gain, qkv_weight, gate_up_weight)


def solution(mesh):
    placed = (P("rep"), P("rep", "tp"), P("tp"), P("rep", "tp"), P("rep", "tp"))
    return jax.shard_map(
        functools.partial(per_device, mesh.shape["rep"], mesh.shape["tp"]),
        mesh=mesh,
        in_specs=placed,
        out_specs=(P("rep", "tp"), P("rep", "tp")),
        check_vma=False,
    )
```
